32 devices in a mesh: arow: 4 (over z), acol: 8 (over y, x, core).
Axes of the slice: x: 2, y: 2, z: 4, core: 2. Of those that a mesh axis runs over, the one named last changes fastest.
Arguments:
- row_data: bfloat16 [65536, 128], P(('arow', 'acol')), may hold values from -96 to 96
- row_baseline: int32 [65536], P(('arow', 'acol')), may hold values from 0 to 131071, as said below
- pair_table: int32 [131072, 2], P(('arow', 'acol')), may hold values from 0 to 2047, as said below
- lengths: int32 [131072], P(('arow', 'acol')), may hold values from 1 to 8
- model_vis: bfloat16 [2048, 2048, 128], P('arow', 'acol'), may hold values from -6 to 6
- gains: float32 [2048, 128], P(('arow', 'acol')), may hold values from -6 to 6
Outputs:
- new_gains: float32 [2048, 128], P(('arow', 'acol'))
The draws below stay inside these ranges and needn't reach their ends.
Inputs may be any that keep to these rules, and one draw needn't show every extreme that they name: `pair_table`: slot j belongs to tile o = j // 4096; its first antenna lies in 512 * (o // 8) to 512 * (o // 8 + 1) - 1, its second in 256 * (o % 8) to 256 * (o % 8 + 1) - 1, and the two differ. `row_baseline`: the rows of one device name slots of one tile at most 256 times; one tile is named exactly 256 times by the rows of every device.
All inputs are finite; a program needn't handle non-finite values.
Results may differ from the reference program's by a relative error of at most 0.0003.
Values may be sent and summed in bfloat16 or wider, within the bound.
A program may use at most 128 MiB of HBM per device.

```python
import jax
import jax.numpy as jnp
from jax import lax

A = 2048
F = 64
ROWS_DEV = 2048
BPO = 4096
AR = 512
AC = 256
CAP = 256
ROWS = 65536
NBW = 131072
DEVICES = 32


def draw_pair_table(key, part):
    index = jnp.arange(NBW, dtype=jnp.int32)
    owner = index // BPO
    blocks = A // AC
    first = owner // blocks * AR + jax.random.randint(jax.random.fold_in(key, 11), (NBW,), 0, AR, dtype=jnp.int32)
    pick = jax.random.randint(jax.random.fold_in(key, 12), (NBW,), 0, AC, dtype=jnp.int32)
    second = owner % blocks * AC + pick
    second = jnp.where(second == first, owner % blocks * AC + (pick + 1) % AC, second)
    return jnp.stack([first, second], axis=1)


def draw_row_baseline(key, part):
    spots = jnp.arange(ROWS_DEV, dtype=jnp.int32)
    flips = jax.random.randint(jax.random.fold_in(key, 21), (DEVICES, ROWS_DEV), 0, 2, dtype=jnp.int32)
    rest = spots[None, :] - CAP
    ranking = jnp.where(spots[None, :] < CAP, 0, 1 + (rest % (DEVICES - 1) + flips) % (DEVICES - 1))
    streams = jax.random.split(jax.random.fold_in(key, 22), DEVICES)
    mixed = jax.vmap(lambda stream, row: row[jax.random.permutation(stream, ROWS_DEV)])(streams, ranking)
    chosen = jax.random.permutation(jax.random.fold_in(key, 23), DEVICES).astype(jnp.int32)
    owner = chosen[mixed]
    pick = jax.random.randint(jax.random.fold_in(key, 24), (DEVICES, ROWS_DEV), 0, BPO, dtype=jnp.int32)
    return (owner * BPO + pick).reshape(ROWS).astype(jnp.int32)


def set_ends(result, stream_key, low, high):
    longest = result.shape.index(max(result.shape))
    spots = []
    for shift in (0, 1):
        where = [jax.random.randint(jax.random.fold_in(stream_key, axis), (), 0, length) for axis, length in enumerate(result.shape)]
        where[longest] = (where[longest] + shift) % result.shape[longest]
        spots.append(tuple(where))
    return result.at[spots[0]].set(low).at[spots[1]].set(high)


def levels(stream_key, shape, cuts, smallest, high):
    gain = 1.0
    for axis_at, shards_of in cuts:
        heights = jax.random.uniform(jax.random.fold_in(jax.random.fold_in(stream_key, 6), axis_at), (shards_of,), jnp.float32, smallest / len(cuts), high / len(cuts))
        gain = gain * jnp.repeat(jnp.exp(heights), shape[axis_at] // shards_of).reshape((-1,) + (1,) * (len(shape) - 1 - axis_at))
    return gain


def noise(stream_key, extent, spread, bound, pieces=(), held_as=jnp.bfloat16):
    entries = jax.random.normal(stream_key, extent, jnp.float32) * spread
    if len(pieces) > 0:
        entries = levels(stream_key, extent, pieces, -0.22, 0.18) * entries
    return jnp.clip(entries, min=-bound, max=bound).astype(held_as)


def setup_inputs(seed: int = 0) -> dict:
    streams_of = jax.random.split(jax.random.key(seed), 7)
    return {
        "row_data": noise(streams_of[0], (ROWS, 2 * F), 16.0, 96.0, ((0, 32),)),
        "row_baseline": draw_row_baseline(jax.random.fold_in(streams_of[6], 71), 0),
        "pair_table": draw_pair_table(jax.random.fold_in(streams_of[6], 71), 0),
        "lengths": set_ends(jax.random.randint(streams_of[3], (NBW,), 1, 9), jax.random.fold_in(streams_of[3], 1), 1, 8).astype(jnp.int32),
        "model_vis": noise(streams_of[4], (A, A, 2 * F), 1.0, 6.0, ((0, 4), (1, 8))),
        "gains": noise(streams_of[5], (A, 2 * F), 1.0, 6.0, ((0, 32),), jnp.float32),
    }


def reference(row_data, row_baseline, pair_table, lengths, model_vis, gains):
    pairs = pair_table[row_baseline]
    first = pairs[:, 0]
    second = pairs[:, 1]
    weight = lengths[row_baseline].astype(jnp.float32)
    terms = weight[:, None] * row_data.astype(jnp.float32)
    nant = gains.shape[0]
    half = gains.shape[1] // 2
    band = nant // 8
    g_re = gains[None, :, :half]
    g_im = gains[None, :, half:]

    def block(index):
        start = index * band
        local = first - start
        inside = (local >= 0) & (local < band)
        spot = jnp.where(inside, local * nant + second, band * nant)
        sums = jnp.zeros((band * nant + 1, 2 * half), jnp.float32).at[spot].add(terms)
        sums = sums[:-1].reshape(band, nant, 2 * half)
        totals = jnp.zeros((band * nant + 1,), jnp.float32).at[spot].add(weight)
        totals = totals[:-1].reshape(band, nant)
        model = lax.dynamic_slice_in_dim(model_vis, start, band, 0)
        m_re = model[..., :half].astype(jnp.float32)
        m_im = model[..., half:].astype(jnp.float32)
        c_re = m_re * g_re + m_im * g_im
        c_im = m_re * g_im - m_im * g_re
        s_re = sums[..., :half]
        s_im = sums[..., half:]
        num = jnp.concatenate([jnp.sum(c_re * s_re - c_im * s_im, axis=1), jnp.sum(c_re * s_im + c_im * s_re, axis=1)], axis=1)
        den = jnp.sum(totals[:, :, None] * (c_re * c_re + c_im * c_im), axis=1)
        return num, den

    nums, dens = lax.map(block, jnp.arange(8, dtype=jnp.int32))
    num = nums.reshape(nant, 2 * half)
    den = dens.reshape(nant, half)
    return jnp.concatenate([num[:, :half] / (den + 1.0), num[:, half:] / (den + 1.0)], axis=1)
```

```python
import functools

import jax
import jax.numpy as jnp
from jax import lax
from jax.experimental import pallas as pl
from jax.experimental.pallas import tpu as pltpu
from jax.sharding import PartitionSpec as P

RIDGE = 1.0
LANES = 128
MESH = pl.DeviceIdType.MESH


def rows_at(ref, start, count):
    return ref[pl.ds(start, count), :]


def route_kernel(
    devices, capacity, slots, rows_ref, base_ref, out_ref, label_ref,
    wide, spread, target, local_id, empty, target_s, local_s, sems,
):
    blocks = base_ref.shape[0]
    count = rows_ref.shape[0]
    empty[...] = jnp.full(empty.shape, slots, jnp.int32)
    fill = pltpu.make_async_copy(empty, label_ref, sems.at[0])
    fill.start()
    order = lax.broadcasted_iota(jnp.int32, (LANES, LANES), 0)
    upper = (order < lax.broadcasted_iota(jnp.int32, (LANES, LANES), 1)).astype(jnp.bfloat16)
    tile = lax.broadcasted_iota(jnp.int32, (devices, LANES), 0)
    before = jnp.zeros((devices, 1), jnp.float32)
    for block in range(blocks):
        slot = base_ref[block : block + 1, :]
        owner = slot // slots
        hit = tile == owner
        hits = jnp.where(hit, 1.0, 0.0)
        within = jnp.dot(hits.astype(jnp.bfloat16), upper, preferred_element_type=jnp.float32)
        ranking = jnp.sum(jnp.where(hit, within + before, 0.0), axis=0, keepdims=True)
        before = before + jnp.sum(hits, axis=1, keepdims=True)
        target[block : block + 1, :] = owner * capacity + ranking.astype(jnp.int32)
        local_id[block : block + 1, :] = slot - owner * slots
    to_target = pltpu.make_async_copy(target, target_s, sems.at[1])
    to_target.start()
    to_local = pltpu.make_async_copy(local_id, local_s, sems.at[2])
    to_local.start()
    wide[...] = rows_ref[...].astype(jnp.float32)
    spread[...] = jnp.zeros_like(spread)
    to_target.wait()
    to_local.wait()
    fill.wait()

    def place_block(block, carry):
        def place(at, carry):
            spot = target_s[block, at]
            label_ref[spot] = local_s[block, at]
            spread[pl.ds(spot, 1), :] = wide[pl.ds(block * LANES + at, 1), :]
            return carry

        return lax.fori_loop(0, LANES, place, carry, unroll=16)

    lax.fori_loop(0, count // LANES, place_block, 0)
    out_ref[...] = spread[...].astype(jnp.bfloat16)


def route(rows, baseline, devices, capacity, slots):
    count, width = rows.shape
    blocks = count // LANES
    total = devices * capacity
    return pl.pallas_call(
        functools.partial(route_kernel, devices, capacity, slots),
        out_shape=(
            jax.ShapeDtypeStruct((total, width), jnp.bfloat16),
            jax.ShapeDtypeStruct((total,), jnp.int32),
        ),
        in_specs=[pl.BlockSpec(memory_space=pltpu.VMEM)] * 2,
        out_specs=(
            pl.BlockSpec(memory_space=pltpu.VMEM),
            pl.BlockSpec(memory_space=pltpu.SMEM),
        ),
        scratch_shapes=[
            pltpu.VMEM((count, width), jnp.float32),
            pltpu.VMEM((total, width), jnp.float32),
            pltpu.VMEM((blocks, LANES), jnp.int32),
            pltpu.VMEM((blocks, LANES), jnp.int32),
            pltpu.VMEM((total,), jnp.int32),
            pltpu.SMEM((blocks, LANES), jnp.int32),
            pltpu.SMEM((blocks, LANES), jnp.int32),
            pltpu.SemaphoreType.DMA((3,)),
        ],
        name="route",
    )(rows, baseline.reshape(blocks, LANES))


def share_kernel(
    row_count, col_count, label_ref, gain_ref, name_ref, column_ref,
    send_sem, recv_sem, gain_send, gain_recv, local_sem,
):
    devices = row_count * col_count
    my_row = lax.axis_index("arow")
    my_col = lax.axis_index("acol")
    me = my_row * col_count + my_col
    barrier = pltpu.get_barrier_semaphore()

    def place(index):
        return (index // col_count, lax.rem(index, col_count))

    def greet(step, carry):
        pl.semaphore_signal(
            barrier, inc=1, device_id=place(lax.rem(me + step, devices)), device_id_type=MESH
        )
        return carry

    lax.fori_loop(1, devices, greet, 0)
    own = pltpu.make_async_copy(label_ref.at[me], name_ref.at[me], local_sem.at[0])
    own.start()
    pl.semaphore_wait(barrier, devices - 1)

    def label_copy(to, slot):
        return pltpu.make_async_remote_copy(
            src_ref=label_ref.at[to],
            dst_ref=name_ref.at[slot],
            send_sem=send_sem.at[to],
            recv_sem=recv_sem.at[slot],
            device_id=place(to),
            device_id_type=MESH,
        )

    def send(step, carry):
        label_copy(lax.rem(me + step, devices), me).start()
        return carry

    lax.fori_loop(1, devices, send, 0)
    column = me // row_count
    part = lax.rem(me, row_count)

    def gain_copy(row, col, slot):
        return pltpu.make_async_remote_copy(
            src_ref=gain_ref,
            dst_ref=column_ref.at[slot],
            send_sem=gain_send.at[row],
            recv_sem=gain_recv.at[slot],
            device_id=(row, col),
            device_id_type=MESH,
        )

    own_gain = pltpu.make_async_copy(gain_ref, column_ref.at[part], local_sem.at[1])
    for row in range(row_count):
        stays = jnp.logical_and(row == my_row, column == my_col)

        @pl.when(jnp.logical_not(stays))
        def _():
            gain_copy(row, column, part).start()

        @pl.when(stays)
        def _():
            own_gain.start()

    for row in range(row_count):
        stays = jnp.logical_and(row == my_row, column == my_col)

        @pl.when(jnp.logical_not(stays))
        def _():
            gain_copy(row, column, part).wait_send()

        @pl.when(stays)
        def _():
            own_gain.wait()

    for slot in range(row_count):
        source = my_col * row_count + slot

        @pl.when(source != me)
        def _():
            gain_copy(0, my_col, slot).wait_recv()

    def finish(step, carry):
        other = lax.rem(me + step, devices)
        label_copy(other, other).wait()
        return carry

    lax.fori_loop(1, devices, finish, 0)
    own.wait()


def share(labels, gains, row_count, col_count):
    devices = row_count * col_count
    return pl.pallas_call(
        functools.partial(share_kernel, row_count, col_count),
        out_shape=(
            jax.ShapeDtypeStruct(labels.shape, jnp.int32),
            jax.ShapeDtypeStruct((row_count,) + gains.shape, jnp.float32),
        ),
        in_specs=[pl.BlockSpec(memory_space=pltpu.VMEM)] * 2,
        out_specs=(pl.BlockSpec(memory_space=pltpu.VMEM),) * 2,
        scratch_shapes=[
            pltpu.SemaphoreType.DMA((devices,)),
            pltpu.SemaphoreType.DMA((devices,)),
            pltpu.SemaphoreType.DMA((row_count,)),
            pltpu.SemaphoreType.DMA((row_count,)),
            pltpu.SemaphoreType.DMA((2,)),
        ],
        compiler_params=pltpu.CompilerParams(collective_id=0, has_side_effects=True),
        name="share",
    )(labels, gains)


def gather_kernel(
    col_block, pairs, chunk, name_ref, table_ref, model_ref, gain_ref, c_ref, info_ref,
    model, gain_rows, picked, sem,
):
    total = c_ref.shape[0]
    width = c_ref.shape[1]
    half = width // 2
    load = pltpu.make_async_copy(model_ref, model, sem)
    load.start()

    def look(at, carry):
        info = table_ref[name_ref[at]]
        info_ref[at] = info
        second = info & (col_block - 1)
        gain_rows[pl.ds(at, 1), :] = gain_ref[pl.ds(second, 1), :]
        return carry

    lax.fori_loop(0, total, look, 0, unroll=16)
    load.wait()

    def piece(number, carry):
        start = number * chunk

        def fetch(at, carry):
            info = info_ref[start + at]
            spot = (info >> 1) & (pairs - 1)
            picked[pl.ds(2 * at + 1 - (info & 1), 2), :] = model[spot].astype(jnp.float32)
            return carry

        lax.fori_loop(0, chunk, fetch, 0, unroll=16)
        m = picked[pl.ds(1, chunk, stride=2), :]
        g = gain_rows[pl.ds(pl.multiple_of(start, chunk), chunk), :]
        a = m * g
        b = m * pltpu.roll(g, half, 1)
        low = lax.broadcasted_iota(jnp.int32, (chunk, width), 1) < half
        c_ref[pl.ds(pl.multiple_of(start, chunk), chunk), :] = jnp.where(
            low, a + pltpu.roll(a, half, 1), pltpu.roll(b, half, 1) - b
        )
        return carry

    lax.fori_loop(0, total // chunk, piece, 0)


def gather(names, table, model_vis, column_gains):
    row_block, col_block, width = model_vis.shape
    pairs = row_block * col_block // 2
    total = names.shape[0]
    chunk = min(512, total)
    return pl.pallas_call(
        functools.partial(gather_kernel, col_block, pairs, chunk),
        out_shape=(
            jax.ShapeDtypeStruct((total, width), jnp.float32),
            jax.ShapeDtypeStruct((total,), jnp.int32),
        ),
        in_specs=[
            pl.BlockSpec(memory_space=pltpu.SMEM),
            pl.BlockSpec(memory_space=pltpu.SMEM),
            pl.BlockSpec(memory_space=pl.ANY),
            pl.BlockSpec(memory_space=pltpu.VMEM),
        ],
        out_specs=(
            pl.BlockSpec(memory_space=pltpu.VMEM),
            pl.BlockSpec(memory_space=pltpu.SMEM),
        ),
        scratch_shapes=[
            pltpu.VMEM((pairs, 2, width), jnp.bfloat16),
            pltpu.VMEM((total, width), jnp.float32),
            pltpu.VMEM((2 * chunk + 8, width), jnp.float32),
            pltpu.SemaphoreType.DMA,
        ],
        compiler_params=pltpu.CompilerParams(vmem_limit_bytes=56 << 20),
        cost_estimate=pl.CostEstimate(
            flops=1 << 20, bytes_accessed=model_vis.size * 2, transcendentals=0
        ),
        name="gather",
    )(names, table, model_vis.reshape(pairs, 2, width), column_gains)


def pick_rows(info, row_block, col_block):
    first = (info // col_block) & (row_block - 1)
    weight = (info // (row_block * col_block)).astype(jnp.float32)
    spots = lax.broadcasted_iota(jnp.int32, (row_block, info.shape[1]), 0)
    return jnp.where(spots == first, weight, 0.0).astype(jnp.bfloat16)


def power_kernel(col_block, info_ref, c_ref, out_ref):
    row_block, width = out_ref.shape
    half = width // 2

    @pl.when(pl.program_id(0) == 0)
    def _():
        out_ref[...] = jnp.zeros_like(out_ref)

    c = c_ref[...]
    power = c * c
    power = power + pltpu.roll(power, half, 1)
    high = power.astype(jnp.bfloat16).astype(jnp.float32)
    low = lax.broadcasted_iota(jnp.int32, power.shape, 1) < half
    values = jnp.where(low, high, power - high).astype(jnp.bfloat16)
    sums = jnp.dot(
        pick_rows(info_ref[0], row_block, col_block), values, preferred_element_type=jnp.float32
    )
    out_ref[...] += sums + pltpu.roll(sums, half, 1)


def product_kernel(col_block, info_ref, c_ref, rows_ref, out_ref):
    row_block, width = out_ref.shape
    half = width // 2

    @pl.when(pl.program_id(0) == 0)
    def _():
        out_ref[...] = jnp.zeros_like(out_ref)

    c = c_ref[...]
    r = rows_ref[...].astype(jnp.float32)
    a = c * r
    b = c * pltpu.roll(r, half, 1)
    low = lax.broadcasted_iota(jnp.int32, c.shape, 1) < half
    product = jnp.where(low, a - pltpu.roll(a, half, 1), b + pltpu.roll(b, half, 1))
    high = product.astype(jnp.bfloat16)
    rest = (product - high.astype(jnp.float32)).astype(jnp.bfloat16)
    values = jnp.concatenate([high, rest], axis=1)
    sums = jnp.dot(
        pick_rows(info_ref[0], row_block, col_block), values, preferred_element_type=jnp.float32
    )
    out_ref[...] += sums[:, :width] + sums[:, width:]


def segment(kernel, name, info, arrays, row_block, col_block):
    total, width = arrays[0].shape
    chunk = min(1024, total)
    steps = total // chunk
    return pl.pallas_call(
        functools.partial(kernel, col_block),
        out_shape=jax.ShapeDtypeStruct((row_block, width), jnp.float32),
        grid=(steps,),
        in_specs=[pl.BlockSpec((1, 1, chunk), lambda i: (i, 0, 0))]
        + [pl.BlockSpec((chunk, width), lambda i: (i, 0))] * len(arrays),
        out_specs=pl.BlockSpec((row_block, width), lambda i: (0, 0)),
        cost_estimate=pl.CostEstimate(
            flops=2 * row_block * total * 2 * width,
            bytes_accessed=total * width * 4,
            transcendentals=0,
        ),
        name=name,
    )(info.reshape(steps, 1, chunk), *arrays)


def collect_kernel(count, divided, *refs):
    if divided:
        part_ref, den_ref, out_ref, held, send_sem, recv_sem = refs
    else:
        part_ref, out_ref, held, send_sem, recv_sem = refs
    me = lax.axis_index("acol")
    barrier = pltpu.get_barrier_semaphore()
    for step in range(1, count):
        pl.semaphore_signal(
            barrier,
            inc=1,
            device_id=(lax.axis_index("arow"), lax.rem(me + step, count)),
            device_id_type=MESH,
        )
    pl.semaphore_wait(barrier, count - 1)

    def copy(to, slot):
        return pltpu.make_async_remote_copy(
            src_ref=part_ref.at[to],
            dst_ref=held.at[slot],
            send_sem=send_sem.at[to],
            recv_sem=recv_sem.at[slot],
            device_id=(lax.axis_index("arow"), to),
            device_id_type=MESH,
        )

    for step in range(1, count):
        copy(lax.rem(me + step, count), me).start()
    total = part_ref[me]
    for step in range(1, count):
        other = lax.rem(me + step, count)
        copy(other, other).wait()
        total = total + held[other]
    if divided:
        total = total / (den_ref[...] + RIDGE)
    out_ref[...] = total


def collect(parts, denominator, count, number):
    rows, width = parts.shape
    share_rows = rows // count
    divided = denominator is not None
    operands = [parts.reshape(count, share_rows, width)] + ([denominator] if divided else [])
    return pl.pallas_call(
        functools.partial(collect_kernel, count, divided),
        out_shape=jax.ShapeDtypeStruct((share_rows, width), jnp.float32),
        in_specs=[pl.BlockSpec(memory_space=pltpu.VMEM)] * len(operands),
        out_specs=pl.BlockSpec(memory_space=pltpu.VMEM),
        scratch_shapes=[
            pltpu.VMEM((count, share_rows, width), jnp.float32),
            pltpu.SemaphoreType.DMA((count,)),
            pltpu.SemaphoreType.DMA((count,)),
        ],
        compiler_params=pltpu.CompilerParams(collective_id=number, has_side_effects=True),
        name="collect" + str(number),
    )(*operands)


def local(row_count, col_count, row_data, row_baseline, pair_table, lengths, model_vis, gains):
    devices = row_count * col_count
    slots = lengths.shape[0]
    capacity = 4 * row_data.shape[0] // devices
    row_block, col_block, width = model_vis.shape
    total = devices * capacity
    my_row = lax.axis_index("arow")
    my_col = lax.axis_index("acol")
    first = pair_table[:, 0] - my_row * row_block
    second = pair_table[:, 1] - my_col * col_block
    table = (lengths * row_block + first) * col_block + second
    table = jnp.concatenate([table, jnp.zeros((LANES,), jnp.int32)])
    outgoing, labels = route(row_data, row_baseline, devices, capacity, slots)
    names, column_gains = share(
        labels.reshape(devices, 1, capacity), gains, row_count, col_count
    )
    outgoing, names = lax.optimization_barrier((outgoing, names))
    arrived = lax.all_to_all(
        outgoing.reshape(devices, capacity, width),
        ("arow", "acol"),
        split_axis=0,
        concat_axis=0,
        tiled=True,
    ).reshape(total, width)
    c, info = gather(
        names.reshape(total), table, model_vis, column_gains.reshape(col_block, width)
    )
    power = segment(power_kernel, "power", info, [c], row_block, col_block)
    denominator = collect(power, None, col_count, 1)
    product = segment(product_kernel, "product", info, [c, arrived], row_block, col_block)
    return collect(product, denominator, col_count, 2)


def solution(mesh):
    placed = (
        P(("arow", "acol"), None),
        P(("arow", "acol")),
        P(("arow", "acol"), None),
        P(("arow", "acol")),
        P("arow", "acol", None),
        P(("arow", "acol"), None),
    )
    return jax.shard_map(
        functools.partial(local, mesh.shape["arow"], mesh.shape["acol"]),
        mesh=mesh,
        in_specs=placed,
        out_specs=P(("arow", "acol"), None),
        check_vma=False,
    )
```

```python
import functools

import jax
import jax.numpy as jnp
from jax import lax
from jax.experimental import pallas as pl
from jax.experimental.pallas import tpu as pltpu
from jax.sharding import PartitionSpec as P

RIDGE = 1.0
LANES = 128
GROUP = 32
WEIGHT_BITS = 4
MESH = pl.DeviceIdType.MESH


def rows_at(ref, start, count):
    return ref[pl.ds(start, count), :]


def route_kernel(
    devices, capacity, slots, rows_ref, base_ref, out_ref, label_ref,
    wide, spread, target, local_id, empty, target_s, local_s, sems,
):
    blocks = base_ref.shape[0]
    count = rows_ref.shape[0]
    empty[...] = jnp.full(empty.shape, slots, jnp.int32)
    fill = pltpu.make_async_copy(empty, label_ref, sems.at[0])
    fill.start()
    order = lax.broadcasted_iota(jnp.int32, (LANES, LANES), 0)
    upper = (order < lax.broadcasted_iota(jnp.int32, (LANES, LANES), 1)).astype(jnp.bfloat16)
    tile = lax.broadcasted_iota(jnp.int32, (devices, LANES), 0)
    before = jnp.zeros((devices, 1), jnp.float32)
    for block in range(blocks):
        slot = base_ref[block : block + 1, :]
        owner = slot // slots
        hit = tile == owner
        hits = jnp.where(hit, 1.0, 0.0)
        within = jnp.dot(hits.astype(jnp.bfloat16), upper, preferred_element_type=jnp.float32)
        ranking = jnp.sum(jnp.where(hit, within + before, 0.0), axis=0, keepdims=True)
        before = before + jnp.sum(hits, axis=1, keepdims=True)
        target[block : block + 1, :] = owner * capacity + ranking.astype(jnp.int32)
        local_id[block : block + 1, :] = slot - owner * slots
    to_target = pltpu.make_async_copy(target, target_s, sems.at[1])
    to_target.start()
    to_local = pltpu.make_async_copy(local_id, local_s, sems.at[2])
    to_local.start()
    wide[...] = rows_ref[...].astype(jnp.float32)
    spread[...] = jnp.zeros_like(spread)
    to_target.wait()
    to_local.wait()
    fill.wait()

    def place_block(block, carry):
        def place(group, carry):
            first = group * GROUP
            spots = [target_s[block, first + k] for k in range(GROUP)]
            ids = [local_s[block, first + k] for k in range(GROUP)]
            held = [
                wide[pl.ds(block * LANES + first + k, 1), :] for k in range(GROUP)
            ]
            for k in range(GROUP):
                label_ref[spots[k]] = ids[k]
                spread[pl.ds(spots[k], 1), :] = held[k]
            return carry

        return lax.fori_loop(0, LANES // GROUP, place, carry)

    lax.fori_loop(0, count // LANES, place_block, 0)
    out_ref[...] = spread[...].astype(jnp.bfloat16)


def route(rows, baseline, devices, capacity, slots):
    count, width = rows.shape
    blocks = count // LANES
    total = devices * capacity
    return pl.pallas_call(
        functools.partial(route_kernel, devices, capacity, slots),
        out_shape=(
            jax.ShapeDtypeStruct((total, width), jnp.bfloat16),
            jax.ShapeDtypeStruct((total,), jnp.int32),
        ),
        in_specs=[pl.BlockSpec(memory_space=pltpu.VMEM)] * 2,
        out_specs=(
            pl.BlockSpec(memory_space=pltpu.VMEM),
            pl.BlockSpec(memory_space=pltpu.SMEM),
        ),
        scratch_shapes=[
            pltpu.VMEM((count, width), jnp.float32),
            pltpu.VMEM((total, width), jnp.float32),
            pltpu.VMEM((blocks, LANES), jnp.int32),
            pltpu.VMEM((blocks, LANES), jnp.int32),
            pltpu.VMEM((total,), jnp.int32),
            pltpu.SMEM((blocks, LANES), jnp.int32),
            pltpu.SMEM((blocks, LANES), jnp.int32),
            pltpu.SemaphoreType.DMA((3,)),
        ],
        name="route",
    )(rows, baseline.reshape(blocks, LANES))


def share_kernel(
    row_count, col_count, label_ref, gain_ref, name_ref, column_ref,
    send_sem, recv_sem, gain_send, gain_recv, local_sem,
):
    devices = row_count * col_count
    my_row = lax.axis_index("arow")
    my_col = lax.axis_index("acol")
    me = my_row * col_count + my_col
    barrier = pltpu.get_barrier_semaphore()

    def place(index):
        return (index // col_count, lax.rem(index, col_count))

    def greet(step, carry):
        pl.semaphore_signal(
            barrier, inc=1, device_id=place(lax.rem(me + step, devices)), device_id_type=MESH
        )
        return carry

    lax.fori_loop(1, devices, greet, 0)
    own = pltpu.make_async_copy(label_ref.at[me], name_ref.at[me], local_sem.at[0])
    own.start()
    pl.semaphore_wait(barrier, devices - 1)

    def label_copy(to, slot):
        return pltpu.make_async_remote_copy(
            src_ref=label_ref.at[to],
            dst_ref=name_ref.at[slot],
            send_sem=send_sem.at[to],
            recv_sem=recv_sem.at[slot],
            device_id=place(to),
            device_id_type=MESH,
        )

    def send(step, carry):
        label_copy(lax.rem(me + step, devices), me).start()
        return carry

    lax.fori_loop(1, devices, send, 0)
    column = me // row_count
    part = lax.rem(me, row_count)

    def gain_copy(row, col, slot):
        return pltpu.make_async_remote_copy(
            src_ref=gain_ref,
            dst_ref=column_ref.at[slot],
            send_sem=gain_send.at[row],
            recv_sem=gain_recv.at[slot],
            device_id=(row, col),
            device_id_type=MESH,
        )

    own_gain = pltpu.make_async_copy(gain_ref, column_ref.at[part], local_sem.at[1])
    for row in range(row_count):
        stays = jnp.logical_and(row == my_row, column == my_col)

        @pl.when(jnp.logical_not(stays))
        def _():
            gain_copy(row, column, part).start()

        @pl.when(stays)
        def _():
            own_gain.start()

    for row in range(row_count):
        stays = jnp.logical_and(row == my_row, column == my_col)

        @pl.when(jnp.logical_not(stays))
        def _():
            gain_copy(row, column, part).wait_send()

        @pl.when(stays)
        def _():
            own_gain.wait()

    for slot in range(row_count):
        source = my_col * row_count + slot

        @pl.when(source != me)
        def _():
            gain_copy(0, my_col, slot).wait_recv()

    def finish(step, carry):
        other = lax.rem(me + step, devices)
        label_copy(other, other).wait()
        return carry

    lax.fori_loop(1, devices, finish, 0)
    own.wait()


def share(labels, gains, row_count, col_count):
    devices = row_count * col_count
    return pl.pallas_call(
        functools.partial(share_kernel, row_count, col_count),
        out_shape=(
            jax.ShapeDtypeStruct(labels.shape, jnp.int32),
            jax.ShapeDtypeStruct((row_count,) + gains.shape, jnp.float32),
        ),
        in_specs=[pl.BlockSpec(memory_space=pltpu.VMEM)] * 2,
        out_specs=(pl.BlockSpec(memory_space=pltpu.VMEM),) * 2,
        scratch_shapes=[
            pltpu.SemaphoreType.DMA((devices,)),
            pltpu.SemaphoreType.DMA((devices,)),
            pltpu.SemaphoreType.DMA((row_count,)),
            pltpu.SemaphoreType.DMA((row_count,)),
            pltpu.SemaphoreType.DMA((2,)),
        ],
        compiler_params=pltpu.CompilerParams(collective_id=0, has_side_effects=True),
        name="share",
    )(labels, gains)


def gather_kernel(
    col_block, chunk, name_ref, table_ref, model_ref, gain_ref, c_ref, info_ref,
    model, pair_gain, gain_rows, picked, sem,
):
    total = c_ref.shape[0]
    width = c_ref.shape[1]
    half = width // 2
    load = pltpu.make_async_copy(model_ref, model, sem)
    load.start()
    shift = col_block.bit_length() + WEIGHT_BITS
    odd = lax.broadcasted_iota(jnp.int32, gain_ref.shape, 0) & 1
    pair_gain[pl.ds(0, col_block, stride=2), :] = jnp.where(odd == 0, gain_ref[...], 0.0)
    pair_gain[pl.ds(1, col_block, stride=2), :] = jnp.where(odd == 1, gain_ref[...], 0.0)

    def look(group, carry):
        first = group * GROUP
        names = [name_ref[first + k] for k in range(GROUP)]
        infos = [table_ref[name] for name in names]
        held = [pair_gain[pl.ds(info & (2 * col_block - 1), 2), :] for info in infos]
        for k in range(GROUP):
            info_ref[first + k] = infos[k]
            gain_rows[pl.ds(2 * (first + k), 2), :] = held[k]
        return carry

    lax.fori_loop(0, total // GROUP, look, 0)
    load.wait()

    def piece(number, carry):
        start = number * chunk

        def fetch(group, carry):
            first = group * GROUP
            infos = [info_ref[start + first + k] for k in range(GROUP)]
            held = [model[info >> shift].astype(jnp.float32) for info in infos]
            for k in range(GROUP):
                picked[pl.ds(2 * (first + k), 2), :] = held[k]
            return carry

        lax.fori_loop(0, chunk // GROUP, fetch, 0)
        at = pl.multiple_of(2 * start, 2 * chunk)
        m_even = picked[pl.ds(0, chunk, stride=2), :]
        m_odd = picked[pl.ds(1, chunk, stride=2), :]
        g_even = gain_rows[pl.ds(at, chunk, stride=2), :]
        g_odd = gain_rows[pl.ds(at + 1, chunk, stride=2), :]
        a = m_even * g_even + m_odd * g_odd
        b = m_even * pltpu.roll(g_even, half, 1) + m_odd * pltpu.roll(g_odd, half, 1)
        low = lax.broadcasted_iota(jnp.int32, (chunk, width), 1) < half
        c_ref[pl.ds(pl.multiple_of(start, chunk), chunk), :] = jnp.where(
            low, a + pltpu.roll(a, half, 1), pltpu.roll(b, half, 1) - b
        )
        return carry

    lax.fori_loop(0, total // chunk, piece, 0)


def gather(names, table, model_vis, column_gains):
    row_block, col_block, width = model_vis.shape
    pairs = row_block * col_block // 2
    total = names.shape[0]
    chunk = min(512, total)
    return pl.pallas_call(
        functools.partial(gather_kernel, col_block, chunk),
        out_shape=(
            jax.ShapeDtypeStruct((total, width), jnp.float32),
            jax.ShapeDtypeStruct((total,), jnp.int32),
        ),
        in_specs=[
            pl.BlockSpec(memory_space=pltpu.SMEM),
            pl.BlockSpec(memory_space=pltpu.SMEM),
            pl.BlockSpec(memory_space=pl.ANY),
            pl.BlockSpec(memory_space=pltpu.VMEM),
        ],
        out_specs=(
            pl.BlockSpec(memory_space=pltpu.VMEM),
            pl.BlockSpec(memory_space=pltpu.SMEM),
        ),
        scratch_shapes=[
            pltpu.VMEM((pairs, 2, width), jnp.bfloat16),
            pltpu.VMEM((2 * col_block, width), jnp.float32),
            pltpu.VMEM((2 * total, width), jnp.float32),
            pltpu.VMEM((2 * chunk, width), jnp.float32),
            pltpu.SemaphoreType.DMA,
        ],
        compiler_params=pltpu.CompilerParams(vmem_limit_bytes=56 << 20),
        cost_estimate=pl.CostEstimate(
            flops=1 << 20, bytes_accessed=model_vis.size * 2, transcendentals=0
        ),
        name="gather",
    )(names, table, model_vis.reshape(pairs, 2, width), column_gains)


def pick_rows(info, row_block, col_block):
    column_bits = col_block.bit_length()
    first = info >> (2 * column_bits + WEIGHT_BITS - 2)
    weight = ((info >> column_bits) & ((1 << WEIGHT_BITS) - 1)).astype(jnp.float32)
    spots = lax.broadcasted_iota(jnp.int32, (row_block, info.shape[1]), 0)
    return jnp.where(spots == first, weight, 0.0).astype(jnp.bfloat16)


def power_kernel(col_block, info_ref, c_ref, out_ref):
    row_block, width = out_ref.shape
    half = width // 2

    @pl.when(pl.program_id(0) == 0)
    def _():
        out_ref[...] = jnp.zeros_like(out_ref)

    c = c_ref[...]
    power = c * c
    power = power + pltpu.roll(power, half, 1)
    high = power.astype(jnp.bfloat16).astype(jnp.float32)
    low = lax.broadcasted_iota(jnp.int32, power.shape, 1) < half
    values = jnp.where(low, high, power - high).astype(jnp.bfloat16)
    sums = jnp.dot(
        pick_rows(info_ref[0], row_block, col_block), values, preferred_element_type=jnp.float32
    )
    out_ref[...] += sums + pltpu.roll(sums, half, 1)


def product_kernel(col_block, info_ref, c_ref, rows_ref, out_ref):
    row_block, width = out_ref.shape
    half = width // 2

    @pl.when(pl.program_id(0) == 0)
    def _():
        out_ref[...] = jnp.zeros_like(out_ref)

    c = c_ref[...]
    r = rows_ref[...].astype(jnp.float32)
    a = c * r
    b = c * pltpu.roll(r, half, 1)
    low = lax.broadcasted_iota(jnp.int32, c.shape, 1) < half
    product = jnp.where(low, a - pltpu.roll(a, half, 1), b + pltpu.roll(b, half, 1))
    high = product.astype(jnp.bfloat16)
    rest = (product - high.astype(jnp.float32)).astype(jnp.bfloat16)
    values = jnp.concatenate([high, rest], axis=1)
    sums = jnp.dot(
        pick_rows(info_ref[0], row_block, col_block), values, preferred_element_type=jnp.float32
    )
    out_ref[...] += sums[:, :width] + sums[:, width:]


def segment(kernel, name, info, arrays, row_block, col_block):
    total, width = arrays[0].shape
    chunk = min(1024, total)
    steps = total // chunk
    return pl.pallas_call(
        functools.partial(kernel, col_block),
        out_shape=jax.ShapeDtypeStruct((row_block, width), jnp.float32),
        grid=(steps,),
        in_specs=[pl.BlockSpec((1, 1, chunk), lambda i: (i, 0, 0))]
        + [pl.BlockSpec((chunk, width), lambda i: (i, 0))] * len(arrays),
        out_specs=pl.BlockSpec((row_block, width), lambda i: (0, 0)),
        cost_estimate=pl.CostEstimate(
            flops=2 * row_block * total * 2 * width,
            bytes_accessed=total * width * 4,
            transcendentals=0,
        ),
        name=name,
    )(info.reshape(steps, 1, chunk), *arrays)


def collect_kernel(
    count, num_ref, den_ref, out_ref, num_held, den_held, num_send, num_recv, den_send, den_recv
):
    me = lax.axis_index("acol")
    barrier = pltpu.get_barrier_semaphore()
    for step in range(1, count):
        pl.semaphore_signal(
            barrier,
            inc=1,
            device_id=(lax.axis_index("arow"), lax.rem(me + step, count)),
            device_id_type=MESH,
        )
    pl.semaphore_wait(barrier, count - 1)

    def copies(to, slot):
        return [
            pltpu.make_async_remote_copy(
                src_ref=part.at[to],
                dst_ref=held.at[slot],
                send_sem=send.at[to],
                recv_sem=recv.at[slot],
                device_id=(lax.axis_index("arow"), to),
                device_id_type=MESH,
            )
            for part, held, send, recv in (
                (den_ref, den_held, den_send, den_recv),
                (num_ref, num_held, num_send, num_recv),
            )
        ]

    for step in range(1, count):
        for copy in copies(lax.rem(me + step, count), me):
            copy.start()
    num = num_ref[me]
    den = den_ref[me]
    for step in range(1, count):
        other = lax.rem(me + step, count)
        for copy in copies(other, other):
            copy.wait()
        num = num + num_held[other]
        den = den + den_held[other]
    out_ref[...] = num / (den + RIDGE)


def collect(numerator, denominator, count):
    rows, width = numerator.shape
    share_rows = rows // count
    shape = (count, share_rows, width)
    return pl.pallas_call(
        functools.partial(collect_kernel, count),
        out_shape=jax.ShapeDtypeStruct((share_rows, width), jnp.float32),
        in_specs=[pl.BlockSpec(memory_space=pltpu.VMEM)] * 2,
        out_specs=pl.BlockSpec(memory_space=pltpu.VMEM),
        scratch_shapes=[pltpu.VMEM(shape, jnp.float32)] * 2
        + [pltpu.SemaphoreType.DMA((count,))] * 4,
        compiler_params=pltpu.CompilerParams(collective_id=1, has_side_effects=True),
        name="collect",
    )(numerator.reshape(shape), denominator.reshape(shape))


def local(row_count, col_count, row_data, row_baseline, pair_table, lengths, model_vis, gains):
    devices = row_count * col_count
    slots = lengths.shape[0]
    capacity = 4 * row_data.shape[0] // devices
    row_block, col_block, width = model_vis.shape
    total = devices * capacity
    my_row = lax.axis_index("arow")
    my_col = lax.axis_index("acol")
    first = pair_table[:, 0] - my_row * row_block
    second = pair_table[:, 1] - my_col * col_block
    pair = first * (col_block // 2) + second // 2
    table = ((pair << WEIGHT_BITS) + lengths) * (2 * col_block) + 2 * second
    table = jnp.concatenate([table, jnp.zeros((LANES,), jnp.int32)])
    outgoing, labels = route(row_data, row_baseline, devices, capacity, slots)
    names, column_gains = share(
        labels.reshape(devices, 1, capacity), gains, row_count, col_count
    )
    outgoing, names = lax.optimization_barrier((outgoing, names))
    arrived = lax.all_to_all(
        outgoing.reshape(devices, capacity, width),
        ("arow", "acol"),
        split_axis=0,
        concat_axis=0,
        tiled=True,
    ).reshape(total, width)
    c, info = gather(
        names.reshape(total), table, model_vis, column_gains.reshape(col_block, width)
    )
    power = segment(power_kernel, "power", info, [c], row_block, col_block)
    product = segment(product_kernel, "product", info, [c, arrived], row_block, col_block)
    return collect(product, power, col_count)


def solution(mesh):
    placed = (
        P(("arow", "acol"), None),
        P(("arow", "acol")),
        P(("arow", "acol"), None),
        P(("arow", "acol")),
        P("arow", "acol", None),
        P(("arow", "acol"), None),
    )
    return jax.shard_map(
        functools.partial(local, mesh.shape["arow"], mesh.shape["acol"]),
        mesh=mesh,
        in_specs=placed,
        out_specs=P(("arow", "acol"), None),
        check_vma=False,
    )
```
